128 devices in a mesh: table: 64 (over x, y, z), mp: 2 (over core).
Axes of the slice: x: 4, y: 4, z: 4, core: 2. Of those that a mesh axis runs over, the one named last changes fastest.
Arguments:
- hash_tables: bfloat16 [2, 65536, 4096], P(None, 'table', 'mp'), may hold values from -6 to 6
- byte_table: bfloat16 [256, 4096], P(None, 'mp'), may hold values from -6 to 6
- byte_ids: int32 [16384], P('table'), may hold values from 0 to 255
- hash_owner: int32 [2, 16384, 1], P(None, 'table'), may hold values from 0 to 63; in each aligned block of 256 rows (0 to 255, 256 to 511, ..., all dimensions but the last counted through in order) at most 8 rows name the same one
- hash_offset: int32 [2, 16384], P(None, 'table'), may hold values from 0 to 1023
- gain: float32 [4096], replicated, may hold values from 0.25 to 1.75
- proj_weight: bfloat16 [4096, 4096], P('table', 'mp'), may hold values from -0.09375 to 0.09375
- cotangent: bfloat16 [16384, 4096], P('table', 'mp'), may hold values from -6 to 6
Outputs:
- projected: bfloat16 [16384, 4096], P('table', 'mp')
- table_grads: bfloat16 [2, 65536, 4096], P(None, 'table', 'mp')
The draws below stay inside these ranges and needn't reach their ends.
Inputs may be any that keep to these rules, and one draw needn't show every extreme that they name: `hash_owner`: within the 256 bytes of one device and one table, no owner is named more than 8 times, a bound that some of these blocks reach.
All inputs are finite; a program needn't handle non-finite values.
Results may differ from the reference program's by a relative error of at most 0.0058.
Values may be sent and summed in bfloat16 or wider, within the bound.
No kernel may reach another device: no remote copies, remote signals or barrier semaphores. Data moves between devices by JAX's collectives and lax.ppermute only.
A program may use at most 128 MiB of HBM per device.

```python
import math
import jax
import jax.numpy as jnp
import numpy as np
from jax import lax

D = 4096
NGRAMS = 2
ROWS_DEV = 1024
VOCAB = 256
TOK_DEV = 256
TOKENS = 16384
ROWS = 65536
CAP = 8
N_TABLE = 64


def plant(drawn, own_key, least, largest):
    spot = [jax.random.randint(jax.random.fold_in(own_key, axis), (), 0, length) for axis, length in enumerate(drawn.shape)]
    longest = drawn.shape.index(max(drawn.shape))
    beside = spot[:longest] + [(spot[longest] + 1) % drawn.shape[longest]] + spot[longest + 1:]
    return drawn.at[tuple(spot)].set(least).at[tuple(beside)].set(largest)


def steps_of(rng, dims, split, least, top_value):
    level = 1.0
    for dim, parts in split:
        steps = jax.random.uniform(jax.random.fold_in(jax.random.fold_in(rng, 6), dim), (parts,), jnp.float32, least / len(split), top_value / len(split))
        level = level * jnp.repeat(jnp.exp(steps), dims[dim] // parts).reshape((-1,) + (1,) * (len(dims) - 1 - dim))
    return level


def cumulative_ranks(number_of, lean):
    portions = [(1 << 20) // math.isqrt(grade ** lean) + 1 for grade in range(1, number_of + 1)]
    deviation = 1 + sum(portions) // (1 << 30)
    return np.cumsum(np.array([max(1, weight // deviation) for weight in portions]))


def ranked(stream_key, dims, amount, slope):
    table = cumulative_ranks(amount, slope)
    lot = jax.random.randint(jax.random.fold_in(stream_key, 1), dims, 0, int(table[amount - 1]))
    standing = jnp.searchsorted(jnp.asarray(table, jnp.int32), lot, side="right")
    return jax.random.permutation(jax.random.fold_in(stream_key, 2), amount)[standing].astype(jnp.int32)


def assign_block(stream_key, own, number, rows, amount, top, limit, lean):
    sequence = jax.random.permutation(stream_key, amount)
    packed, usual = load_shares(amount, rows * top, limit, lean, True), load_shares(amount, rows * top, limit, lean, False)
    places = jnp.arange(amount)

    def named(lengths, turn):
        used = int((lengths > 0).sum())
        fixed = max(1, used // 4)
        moved = fixed + (places - fixed + turn * (used - fixed)) % max(1, amount - fixed)
        return jnp.zeros((amount,), jnp.int32).at[sequence[jnp.where(places < fixed, places, moved)]].set(jnp.asarray(lengths, jnp.int32))

    lengths = jnp.where(number % 4 == 0, named(packed, number // 4), named(usual, number - number // 4 - 1))
    mixed = jax.random.permutation(jax.random.fold_in(own, 3), amount)
    donor, receiver = mixed[0:amount // 2 * 2:2], mixed[1:amount // 2 * 2:2]
    room = jnp.minimum(lengths[donor] - 1, limit - lengths[receiver]) // 2
    room = jnp.where((donor == sequence[0]) | (receiver == sequence[0]) | (lengths[receiver] == 0), 0, jnp.maximum(room, 0))
    moved = jax.random.randint(jax.random.fold_in(own, 4), (amount // 2,), 0, 1 << 20) % (room + 1)
    lengths = lengths.at[donor].add(-moved).at[receiver].add(moved)
    members = jnp.searchsorted(jnp.cumsum(lengths), jnp.arange(rows * top), side="right").astype(jnp.int32)
    grid = members.reshape(top, rows).T
    grid = grid[jax.random.permutation(jax.random.fold_in(own, 1), rows)]
    turn = jax.random.randint(jax.random.fold_in(own, 2), (rows, 1), 0, top)
    return jnp.take_along_axis(grid, (jnp.arange(top)[None, :] + turn) % top, axis=1)


def load_shares(number_of, total, limit, slope, full):
    portions = [(1 << 20) // math.isqrt(grade ** slope) + 1 for grade in range(1, number_of + 1)]
    largest = limit if full else min(limit, max(-(-total // number_of), total * portions[0] // sum(portions)))
    least = 1 if total - largest >= number_of - 1 else 0
    counts, surplus = [largest] + [least] * (number_of - 1), total - largest - least * (number_of - 1)
    while surplus > 0:
        movable = [i for i in range(1, number_of) if counts[i] < largest] or [i for i in range(1, number_of) if counts[i] < limit]
        mass, remaining = sum([portions[i] for i in movable]), surplus
        for i in movable:
            extra = min(limit - counts[i], max(1, remaining * portions[i] // mass), surplus)
            counts[i] = counts[i] + extra
            surplus = surplus - extra
    return np.array(counts)


def noise(stream_key, shape, scale, reach, pieces=(), kind=jnp.bfloat16):
    array = jax.random.normal(stream_key, shape, jnp.float32) * scale
    if len(pieces) > 0:
        array = steps_of(stream_key, shape, pieces, -0.22, 0.18) * array
    return jnp.clip(array, min=-reach, max=reach).astype(kind)


def setup_inputs(seed: int = 0) -> dict:
    keys = jax.random.split(jax.random.key(seed), 9)
    hash_tables = noise(keys[0], (NGRAMS, ROWS, D), 1.0, 6.0, ((1, 64), (2, 2)))
    byte_table = noise(keys[1], (VOCAB, D), 1.0, 6.0, ((1, 2),))
    byte_ids = plant(ranked(keys[2], (TOKENS,), VOCAB, 2), jax.random.fold_in(keys[2], 3), 0, VOCAB - 1).astype(jnp.int32)
    hash_owner_keys = jax.random.split(jax.random.fold_in(keys[3], 1), NGRAMS * TOKENS // TOK_DEV)
    hash_owner_turns = jax.random.permutation(jax.random.fold_in(keys[3], 3), NGRAMS * TOKENS // TOK_DEV)
    hash_owner = jax.vmap(lambda own, number: assign_block(jax.random.fold_in(keys[3], 2), own, number, TOK_DEV, N_TABLE, 1, CAP, 2))(hash_owner_keys, hash_owner_turns).reshape((NGRAMS, TOKENS, 1))
    hash_offset = plant(jax.random.randint(keys[4], (NGRAMS, TOKENS), 0, ROWS_DEV), jax.random.fold_in(keys[4], 1), 0, ROWS_DEV - 1).astype(jnp.int32)
    gain = jnp.clip(1.0 + 0.15 * jax.random.normal(keys[5], (D,), jnp.float32), 0.25, 1.75)
    proj_weight = noise(keys[6], (D, D), D ** -0.5, 0.09375, ((0, 64), (1, 2)))
    cotangent = noise(keys[7], (TOKENS, D), 1.0, 6.0, ((0, 64), (1, 2)))
    return {"hash_tables": hash_tables, "byte_table": byte_table, "byte_ids": byte_ids, "hash_owner": hash_owner, "hash_offset": hash_offset, "gain": gain, "proj_weight": proj_weight, "cotangent": cotangent}


eps = 1e-05

def reference(hash_tables, byte_table, byte_ids, hash_owner, hash_offset, gain, proj_weight, cotangent):
    hashed = (hash_owner[:, :, 0] * ROWS_DEV + hash_offset).astype(jnp.int32)
    summed = byte_table[byte_ids].astype(jnp.float32)
    for k in range(NGRAMS):
        summed = summed + hash_tables[k][hashed[k]].astype(jnp.float32)
    embedded = summed.astype(jnp.bfloat16)
    values = embedded.astype(jnp.float32)
    scale = lax.rsqrt(lax.optimization_barrier(jnp.mean(values * values, axis=1, keepdims=True)) + eps)
    normed = (values * scale * gain[None, :]).astype(jnp.bfloat16)
    projected = jnp.dot(normed, proj_weight, preferred_element_type=jnp.float32).astype(jnp.bfloat16)
    dnormed = lax.dot_general(cotangent, proj_weight, (((1,), (1,)), ((), ())), preferred_element_type=jnp.float32)
    scaled = dnormed * gain[None, :]
    inner = lax.optimization_barrier(jnp.mean(values * scaled, axis=1, keepdims=True))
    dembed = (scale * scaled - values * scale * scale * scale * inner).astype(jnp.bfloat16)
    grads = []
    for k in range(NGRAMS):
        total = jnp.zeros((ROWS, D), jnp.float32).at[hashed[k]].add(dembed.astype(jnp.float32))
        grads.append(total.astype(jnp.bfloat16))
    return (projected, jnp.stack(grads))
```

```python
import functools
import jax
import jax.numpy as jnp
from jax import lax
from jax.experimental import pallas as pl
from jax.experimental.pallas import tpu as pltpu
from jax.sharding import PartitionSpec as P

eps = 1e-05
f32, bf16, i32 = jnp.float32, jnp.bfloat16, jnp.int32
LANES = 128


def iota(shape, dim):
    return lax.broadcasted_iota(i32, shape, dim)


def dot(a, b, ca, cb):
    return lax.dot_general(a, b, (((ca,), (cb,)), ((), ())), preferred_element_type=f32)


def route_body(owner_ref, offset_ref, wanted_ref, slot_ref, *, groups, cap):
    ngram, tokens = owner_ref.shape
    earlier = (iota((tokens, tokens), 0) < iota((tokens, tokens), 1)).astype(f32).astype(bf16)
    lane = iota((groups, LANES), 1)
    wanted = jnp.full((groups, LANES), -1, i32)
    for k in range(ngram):
        owner = owner_ref[k : k + 1, :]
        offset = offset_ref[k : k + 1, :]
        mine = jnp.broadcast_to(owner, (groups, tokens)) == iota((groups, tokens), 0)
        before = dot(mine.astype(f32).astype(bf16), earlier, 1, 0).astype(i32)
        rank = jnp.sum(jnp.where(mine, before, 0), axis=0, keepdims=True)
        slot_ref[k : k + 1, :] = owner * (ngram * cap) + k * cap + rank
        for r in range(cap):
            hit = jnp.where(mine & (before == r), offset + 1, 0)
            value = jnp.sum(hit, axis=1, keepdims=True) - 1
            wanted = jnp.where(lane == k * cap + r, value, wanted)
    wanted_ref[...] = wanted


def route(owner, offset, groups, cap):
    ngram, tokens = owner.shape
    return pl.pallas_call(
        functools.partial(route_body, groups=groups, cap=cap),
        out_shape=(
            jax.ShapeDtypeStruct((groups, LANES), i32),
            jax.ShapeDtypeStruct((ngram, tokens), i32),
        ),
        name="route",
    )(owner, offset)


def row_picks(asked, k, cap, rows):
    groups = asked.shape[0]
    total = groups * cap
    spread = (iota((total, groups), 0) // cap == iota((total, groups), 1)).astype(f32).astype(bf16)
    code = asked + 1
    high = (code >> 5).astype(f32).astype(bf16)
    low = (code & 31).astype(f32).astype(bf16)
    codes = dot(spread, high, 1, 0) * 32.0 + dot(spread, low, 1, 0)
    place = iota((total, LANES), 1) == k * cap + iota((total, LANES), 0) % cap
    column = jnp.sum(jnp.where(place, codes, 0.0), axis=1, keepdims=True).astype(i32) - 1
    return (column == iota((total, rows), 1)).astype(f32).astype(bf16)


def lookup_body(asked_ref, table_ref, out_ref, picks_ref, *, cap):
    k = pl.program_id(0)
    rows = table_ref.shape[1]

    @pl.when(pl.program_id(1) == 0)
    def _():
        picks_ref[...] = row_picks(asked_ref[...], k, cap, rows)

    out = dot(picks_ref[...], table_ref[0], 1, 0).astype(bf16)
    out_ref[...] = out.reshape(out_ref.shape)


def lookup(asked, tables, cap, block):
    groups = asked.shape[0]
    ngram, rows, width = tables.shape
    return pl.pallas_call(
        functools.partial(lookup_body, cap=cap),
        grid=(ngram, width // block),
        in_specs=[
            pl.BlockSpec((groups, LANES), lambda k, j: (0, 0)),
            pl.BlockSpec((1, rows, block), lambda k, j: (k, 0, j)),
        ],
        out_specs=pl.BlockSpec((groups, 1, cap, block), lambda k, j: (0, k, 0, j)),
        out_shape=jax.ShapeDtypeStruct((groups, ngram, cap, width), bf16),
        scratch_shapes=[pltpu.VMEM((groups * cap, rows), bf16)],
        name="lookup",
    )(asked, tables)


def slot_picks(slot, slots):
    ngram, tokens = slot.shape
    place = iota((slots, tokens), 0)
    hit = place == slot[0:1, :]
    for k in range(1, ngram):
        hit = hit | (place == slot[k : k + 1, :])
    return hit.astype(f32).astype(bf16)


def combine_body(slot_ref, ids_ref, fetched_ref, bytes_ref, out_ref, square_ref, picks_ref, codes_ref):
    slots, tokens = picks_ref.shape

    @pl.when(pl.program_id(0) == 0)
    def _():
        picks_ref[...] = slot_picks(slot_ref[...], slots)
        vocab = codes_ref.shape[0]
        codes_ref[...] = (iota((vocab, tokens), 0) == ids_ref[...]).astype(f32).astype(bf16)
        square_ref[...] = jnp.zeros(square_ref.shape, f32)

    block = out_ref.shape[1]
    fetched = fetched_ref[...].reshape(slots, block)
    summed = dot(picks_ref[...], fetched, 0, 0) + dot(codes_ref[...], bytes_ref[...], 0, 0)
    embedded = summed.astype(bf16)
    out_ref[...] = embedded
    values = embedded.astype(f32)
    square_ref[...] += jnp.sum(values * values, axis=1, keepdims=True)


def combine(slot, ids, fetched, byte_table, block):
    groups, ngram, cap, width = fetched.shape
    tokens = slot.shape[1]
    vocab = byte_table.shape[0]
    slots = groups * ngram * cap
    return pl.pallas_call(
        combine_body,
        grid=(width // block,),
        in_specs=[
            pl.BlockSpec((ngram, tokens), lambda j: (0, 0)),
            pl.BlockSpec((1, tokens), lambda j: (0, 0)),
            pl.BlockSpec((groups, ngram, cap, block), lambda j: (0, 0, 0, j)),
            pl.BlockSpec((vocab, block), lambda j: (0, j)),
        ],
        out_specs=(
            pl.BlockSpec((tokens, block), lambda j: (0, j)),
            pl.BlockSpec((tokens, 1), lambda j: (0, 0)),
        ),
        out_shape=(
            jax.ShapeDtypeStruct((tokens, width), bf16),
            jax.ShapeDtypeStruct((tokens, 1), f32),
        ),
        scratch_shapes=[pltpu.VMEM((slots, tokens), bf16), pltpu.VMEM((vocab, tokens), bf16)],
        name="combine",
    )(slot, ids.reshape(1, tokens), fetched, byte_table)


def dispatch_body(slot_ref, scaled_ref, embedded_ref, scale_ref, inner_ref, out_ref, picks_ref):
    slots, tokens = picks_ref.shape

    @pl.when(pl.program_id(0) == 0)
    def _():
        picks_ref[...] = slot_picks(slot_ref[...], slots)

    scale = scale_ref[...]
    values = embedded_ref[...].astype(f32)
    dembed = scale * scaled_ref[...] - values * (scale * scale * scale * inner_ref[...])
    out = dot(picks_ref[...], dembed.astype(bf16), 1, 0).astype(bf16)
    out_ref[...] = out.reshape(out_ref.shape)


def dispatch(slot, scaled, embedded, scale, inner, groups, cap, block):
    ngram, tokens = slot.shape
    width = embedded.shape[1]
    slots = groups * ngram * cap
    return pl.pallas_call(
        dispatch_body,
        grid=(width // block,),
        in_specs=[
            pl.BlockSpec((ngram, tokens), lambda j: (0, 0)),
            pl.BlockSpec((tokens, block), lambda j: (0, j)),
            pl.BlockSpec((tokens, block), lambda j: (0, j)),
            pl.BlockSpec((tokens, 1), lambda j: (0, 0)),
            pl.BlockSpec((tokens, 1), lambda j: (0, 0)),
        ],
        out_specs=pl.BlockSpec((groups, ngram, cap, block), lambda j: (0, 0, 0, j)),
        out_shape=jax.ShapeDtypeStruct((groups, ngram, cap, width), bf16),
        scratch_shapes=[pltpu.VMEM((slots, tokens), bf16)],
        name="dispatch",
    )(slot, scaled, embedded, scale, inner)


def accumulate_body(asked_ref, arrived_ref, out_ref, picks_ref, *, cap):
    k = pl.program_id(0)
    rows = out_ref.shape[1]
    groups = asked_ref.shape[0]

    @pl.when(pl.program_id(1) == 0)
    def _():
        picks_ref[...] = row_picks(asked_ref[...], k, cap, rows)

    arrived = arrived_ref[...].reshape(groups * cap, arrived_ref.shape[-1])
    out_ref[0] = dot(picks_ref[...], arrived, 0, 0).astype(bf16)


def accumulate(asked, arrived, rows, block):
    groups, ngram, cap, width = arrived.shape
    return pl.pallas_call(
        functools.partial(accumulate_body, cap=cap),
        grid=(ngram, width // block),
        in_specs=[
            pl.BlockSpec((groups, LANES), lambda k, j: (0, 0)),
            pl.BlockSpec((groups, 1, cap, block), lambda k, j: (0, k, 0, j)),
        ],
        out_specs=pl.BlockSpec((1, rows, block), lambda k, j: (k, 0, j)),
        out_shape=jax.ShapeDtypeStruct((ngram, rows, width), bf16),
        scratch_shapes=[pltpu.VMEM((groups * cap, rows), bf16)],
        name="accumulate",
    )(asked, arrived)


def exchange(array, axis):
    return lax.all_to_all(array, axis, split_axis=0, concat_axis=0, tiled=True)


def swapped(array):
    return lax.ppermute(array, "mp", [(0, 1), (1, 0)])


def on_device(
    hash_tables, byte_table, byte_ids, hash_owner, hash_offset, gain, proj_weight, cotangent
):
    groups = lax.axis_size("table")
    half = lax.axis_index("mp")
    ngram, rows, width = hash_tables.shape
    tokens = byte_ids.shape[0]
    full_width = gain.shape[0]
    cap = 2 * tokens // groups
    block = 512

    weight = lax.all_gather(proj_weight, "table", axis=0, tiled=True)
    wanted, slot = route(hash_owner[:, :, 0], hash_offset, groups, cap)
    asked = exchange(wanted.reshape(groups, 1, LANES), "table").reshape(groups, LANES)
    looked = lookup(asked, hash_tables, cap, block)
    fetched = exchange(looked, "table")
    embedded, square = combine(slot, byte_ids, fetched, byte_table, block)

    partial = dot(cotangent, weight, 1, 1)
    low, high = partial[:, :width], partial[:, width:]
    given = jnp.where(half == 0, high, low).astype(bf16)
    kept = jnp.where(half == 0, low, high)
    gain_half = lax.dynamic_slice_in_dim(gain, half * width, width)
    scaled = (kept + swapped(given).astype(f32)) * gain_half[None, :]
    inner = jnp.sum(embedded.astype(f32) * scaled, axis=1)
    sums = jnp.stack([square[:, 0], inner])
    sums = sums + swapped(sums)
    scale = lax.rsqrt(sums[0] / full_width + eps)[:, None]
    inner = (sums[1] / full_width)[:, None]
    sends = dispatch(slot, scaled, embedded, scale, inner, groups, cap, block)
    arrived = exchange(sends, "table")

    other = swapped(embedded)
    whole = jnp.where(
        half == 0,
        jnp.concatenate([embedded, other], axis=1),
        jnp.concatenate([other, embedded], axis=1),
    )
    normed = (whole.astype(f32) * scale * gain[None, :]).astype(bf16)
    projected = dot(normed, weight, 1, 0).astype(bf16)
    table_grads = accumulate(asked, arrived, rows, block)
    return (projected, table_grads)


def solution(mesh):
    return jax.shard_map(
        on_device,
        mesh=mesh,
        in_specs=(
            P(None, "table", "mp"),
            P(None, "mp"),
            P("table"),
            P(None, "table", None),
            P(None, "table"),
            P(),
            P("table", "mp"),
            P("table", "mp"),
        ),
        out_specs=(P("table", "mp"), P(None, "table", "mp")),
        check_vma=False,
    )
```

```python
import functools
import jax
import jax.numpy as jnp
from jax import lax
from jax.experimental import pallas as pl
from jax.experimental.pallas import tpu as pltpu
from jax.sharding import Mesh, PartitionSpec as P

eps = 1e-05
f32, bf16, i32 = jnp.float32, jnp.bfloat16, jnp.int32
LANES = 128
SPAN = 256
AXES = ("x", "y", "z")


def iota(shape, dim):
    return lax.broadcasted_iota(i32, shape, dim)


def dot(a, b, ca, cb):
    return lax.dot_general(a, b, (((ca,), (cb,)), ((), ())), preferred_element_type=f32)


def route_body(owner_ref, offset_ref, wanted_ref, slot_ref, *, groups, cap):
    ngram, _, tokens = owner_ref.shape
    earlier = (iota((tokens, tokens), 0) < iota((tokens, tokens), 1)).astype(f32).astype(bf16)
    lane = iota((groups, LANES), 1)
    wanted = jnp.full((groups, LANES), -1, i32)
    for k in range(ngram):
        owner = owner_ref[k]
        offset = offset_ref[k : k + 1, :]
        mine = jnp.broadcast_to(owner, (groups, tokens)) == iota((groups, tokens), 0)
        before = dot(mine.astype(f32).astype(bf16), earlier, 1, 0).astype(i32)
        rank = jnp.sum(jnp.where(mine, before, 0), axis=0, keepdims=True)
        slot_ref[k : k + 1, :] = owner * (ngram * cap) + k * cap + rank
        for r in range(cap):
            hit = jnp.where(mine & (before == r), offset + 1, 0)
            value = jnp.sum(hit, axis=1, keepdims=True) - 1
            wanted = jnp.where(lane == k * cap + r, value, wanted)
    wanted_ref[...] = wanted


def route(owner, offset, groups, cap):
    ngram, _, tokens = owner.shape
    return pl.pallas_call(
        functools.partial(route_body, groups=groups, cap=cap),
        out_shape=(
            jax.ShapeDtypeStruct((groups, LANES), i32),
            jax.ShapeDtypeStruct((ngram, tokens), i32),
        ),
        name="route",
    )(owner, offset)


def row_picks(asked, k, cap, rows):
    groups = asked.shape[0]
    total = groups * cap
    spread = (iota((total, groups), 0) // cap == iota((total, groups), 1)).astype(f32).astype(bf16)
    code = asked + 1
    high = (code >> 5).astype(f32).astype(bf16)
    low = (code & 31).astype(f32).astype(bf16)
    codes = dot(spread, high, 1, 0) * 32.0 + dot(spread, low, 1, 0)
    place = iota((total, LANES), 1) == k * cap + iota((total, LANES), 0) % cap
    column = jnp.sum(jnp.where(place, codes, 0.0), axis=1, keepdims=True).astype(i32) - 1
    return (column == iota((total, rows), 1)).astype(f32).astype(bf16)


def lookup_body(asked_ref, table_ref, out_ref, picks_ref, *, cap):
    k = pl.program_id(0)
    rows = table_ref.shape[1]

    @pl.when(pl.program_id(1) == 0)
    def _():
        picks_ref[...] = row_picks(asked_ref[...], k, cap, rows)

    out = dot(picks_ref[...], table_ref[0], 1, 0).astype(bf16)
    out_ref[...] = out.reshape(out_ref.shape)


def lookup(asked, tables, cap, block):
    groups = asked.shape[0]
    ngram, rows, width = tables.shape
    return pl.pallas_call(
        functools.partial(lookup_body, cap=cap),
        grid=(ngram, width // block),
        in_specs=[
            pl.BlockSpec((groups, LANES), lambda k, j: (0, 0)),
            pl.BlockSpec((1, rows, block), lambda k, j: (k, 0, j)),
        ],
        out_specs=pl.BlockSpec((groups, 1, cap, block), lambda k, j: (0, k, 0, j)),
        out_shape=jax.ShapeDtypeStruct((groups, ngram, cap, width), bf16),
        scratch_shapes=[pltpu.VMEM((groups * cap, rows), bf16)],
        name="lookup",
    )(asked, tables)


def slot_columns(slot_ref, slots):
    ngram, tokens = slot_ref.shape
    filled = jnp.concatenate([slot_ref[...], jnp.zeros((8 - ngram, tokens), i32)], axis=0)
    columns = filled.astype(f32).T.astype(i32)
    place = iota((tokens, slots), 1)
    hit = place == columns[:, 0:1]
    for k in range(1, ngram):
        hit = hit | (place == columns[:, k : k + 1])
    return hit.astype(f32).astype(bf16)


def side_by_side(ref):
    return jnp.concatenate([ref[i] for i in range(ref.shape[0])], axis=1)


def combine_body(
    slot_ref, ids_ref, fetched_ref, bytes_ref, dnormed_ref, gain_ref, out_ref, sums_ref, picks_ref, codes_ref
):
    tokens, slots = picks_ref.shape

    @pl.when(pl.program_id(0) == 0)
    def _():
        picks_ref[...] = slot_columns(slot_ref, slots)
        vocab = codes_ref.shape[0]
        codes_ref[...] = (iota((vocab, tokens), 0) == ids_ref[...]).astype(f32).astype(bf16)
        sums_ref[...] = jnp.zeros(sums_ref.shape, f32)

    block = fetched_ref.shape[-1]
    fetched = fetched_ref[...].reshape(slots, block)
    summed = dot(picks_ref[...], fetched, 1, 0) + dot(codes_ref[...], bytes_ref[...], 0, 0)
    embedded = summed.astype(bf16)
    for i in range(block // SPAN):
        out_ref[i] = embedded[:, i * SPAN : (i + 1) * SPAN]
    values = embedded.astype(f32)
    scaled = side_by_side(dnormed_ref).astype(f32) * gain_ref[...]
    square = jnp.sum(values * values, axis=1, keepdims=True)
    inner = jnp.sum(values * scaled, axis=1, keepdims=True)
    sums_ref[...] += jnp.where(iota(sums_ref.shape, 1) == 0, square, inner)


def combine(slot, ids, fetched, byte_table, dnormed, gain, block):
    groups, ngram, cap, width = fetched.shape
    tokens = slot.shape[1]
    vocab = byte_table.shape[0]
    slots = groups * ngram * cap
    return pl.pallas_call(
        combine_body,
        grid=(width // block,),
        in_specs=[
            pl.BlockSpec((ngram, tokens), lambda j: (0, 0)),
            pl.BlockSpec((1, tokens), lambda j: (0, 0)),
            pl.BlockSpec((groups, ngram, cap, block), lambda j: (0, 0, 0, j)),
            pl.BlockSpec((vocab, block), lambda j: (0, j)),
            pl.BlockSpec((block // SPAN, tokens, SPAN), lambda j: (j, 0, 0)),
            pl.BlockSpec((1, block), lambda j: (0, j)),
        ],
        out_specs=(
            pl.BlockSpec((block // SPAN, tokens, SPAN), lambda j: (j, 0, 0)),
            pl.BlockSpec((tokens, LANES), lambda j: (0, 0)),
        ),
        out_shape=(
            jax.ShapeDtypeStruct((width // SPAN, tokens, SPAN), bf16),
            jax.ShapeDtypeStruct((tokens, LANES), f32),
        ),
        scratch_shapes=[pltpu.VMEM((tokens, slots), bf16), pltpu.VMEM((vocab, tokens), bf16)],
        name="combine",
    )(slot, ids.reshape(1, tokens), fetched, byte_table, dnormed, gain)


def dispatch_body(
    slot_ref, dnormed_ref, gain_ref, embedded_ref, mine_ref, other_ref, out_ref, picks_ref, *, full_width
):
    slots, tokens = picks_ref.shape

    @pl.when(pl.program_id(0) == 0)
    def _():
        place = iota((slots, tokens), 0)
        hit = place == slot_ref[0:1, :]
        for k in range(1, slot_ref.shape[0]):
            hit = hit | (place == slot_ref[k : k + 1, :])
        picks_ref[...] = hit.astype(f32).astype(bf16)

    means = (mine_ref[...] + other_ref[...]) * (1.0 / full_width)
    scale = lax.rsqrt(means[:, 0:1] + eps)
    inner = means[:, 1:2]
    values = side_by_side(embedded_ref).astype(f32)
    scaled = side_by_side(dnormed_ref).astype(f32) * gain_ref[...]
    dembed = scale * scaled - values * (scale * scale * scale * inner)
    out = dot(picks_ref[...], dembed.astype(bf16), 1, 0).astype(bf16)
    out_ref[...] = out.reshape(out_ref.shape)


def dispatch(slot, dnormed, gain, embedded, mine, other, groups, cap, full_width, block):
    ngram, tokens = slot.shape
    width = embedded.shape[0] * SPAN
    slots = groups * ngram * cap
    return pl.pallas_call(
        functools.partial(dispatch_body, full_width=full_width),
        grid=(width // block,),
        in_specs=[
            pl.BlockSpec((ngram, tokens), lambda j: (0, 0)),
            pl.BlockSpec((block // SPAN, tokens, SPAN), lambda j: (j, 0, 0)),
            pl.BlockSpec((1, block), lambda j: (0, j)),
            pl.BlockSpec((block // SPAN, tokens, SPAN), lambda j: (j, 0, 0)),
            pl.BlockSpec((tokens, LANES), lambda j: (0, 0)),
            pl.BlockSpec((tokens, LANES), lambda j: (0, 0)),
        ],
        out_specs=pl.BlockSpec((groups, ngram, cap, block), lambda j: (0, 0, 0, j)),
        out_shape=jax.ShapeDtypeStruct((groups, ngram, cap, width), bf16),
        scratch_shapes=[pltpu.VMEM((slots, tokens), bf16)],
        name="dispatch",
    )(slot, dnormed, gain, embedded, mine, other)


def accumulate_body(asked_ref, arrived_ref, out_ref, picks_ref, *, cap):
    k = pl.program_id(0)
    rows = out_ref.shape[1]
    groups = asked_ref.shape[0]
    total = groups * cap

    @pl.when(pl.program_id(1) == 0)
    def _():
        spread = (iota((total, groups), 0) // cap == iota((total, groups), 1)).astype(f32).astype(bf16)
        code = asked_ref[...] + 1
        high = (code >> 5).astype(f32).astype(bf16)
        low = (code & 31).astype(f32).astype(bf16)
        codes = dot(high, spread, 0, 1) * 32.0 + dot(low, spread, 0, 1)
        place = iota((LANES, total), 0) == k * cap + iota((LANES, total), 1) % cap
        line = jnp.sum(jnp.where(place, codes, 0.0), axis=0, keepdims=True).astype(i32) - 1
        picks_ref[...] = (iota((rows, total), 0) == line).astype(f32).astype(bf16)

    arrived = arrived_ref[...].reshape(total, arrived_ref.shape[-1])
    out_ref[0] = dot(picks_ref[...], arrived, 1, 0).astype(bf16)


def accumulate(asked, arrived, rows, block):
    groups, ngram, cap, width = arrived.shape
    return pl.pallas_call(
        functools.partial(accumulate_body, cap=cap),
        grid=(ngram, width // block),
        in_specs=[
            pl.BlockSpec((groups, LANES), lambda k, j: (0, 0)),
            pl.BlockSpec((groups, 1, cap, block), lambda k, j: (0, k, 0, j)),
        ],
        out_specs=pl.BlockSpec((1, rows, block), lambda k, j: (k, 0, j)),
        out_shape=jax.ShapeDtypeStruct((ngram, rows, width), bf16),
        scratch_shapes=[pltpu.VMEM((rows, groups * cap), bf16)],
        name="accumulate",
    )(asked, arrived)


def exchange(array):
    return lax.all_to_all(array, AXES, split_axis=0, concat_axis=0, tiled=True)


def swapped(array):
    return lax.ppermute(array, "mp", [(0, 1), (1, 0)])


def shifted(array, turned, by):
    pairs = []
    for x in range(4):
        for y in range(4):
            for c in range(2):
                along_x = (c == 0) != turned
                to = ((x + by) % 4, y) if along_x else (x, (y + by) % 4)
                pairs.append(((x * 4 + y) * 2 + c, (to[0] * 4 + to[1]) * 2 + c))
    return lax.ppermute(array, ("x", "y", "mp"), pairs)


def shifted_z(array, by):
    return lax.ppermute(array, "z", [(i, (i + by) % 4) for i in range(4)])


def joined(blocks, here, dim):
    shape = list(blocks[0][0].shape)
    shape.insert(dim, 4)
    whole = jnp.zeros(shape, blocks[0][0].dtype)
    for block, away in blocks:
        whole = lax.dynamic_update_slice_in_dim(
            whole, jnp.expand_dims(block, dim), (here + away) % 4, dim
        )
    return whole


def product_body(*refs):
    cots, weight_ref, outs = refs[:4], refs[4], refs[5:]
    for cot_ref, out_ref in zip(cots, outs, strict=True):
        out_ref[...] = dot(cot_ref[...], weight_ref[...], 1, 1).astype(bf16)


def product(cots, weight, block):
    tokens, width = cots[0].shape
    rows = weight.shape[0]
    return pl.pallas_call(
        product_body,
        grid=(rows // block,),
        in_specs=[pl.BlockSpec((tokens, width), lambda j: (0, 0)) for _ in cots]
        + [pl.BlockSpec((block, width), lambda j: (j, 0))],
        out_specs=[pl.BlockSpec((tokens, block), lambda j: (0, j)) for _ in cots],
        out_shape=[jax.ShapeDtypeStruct((tokens, rows), bf16) for _ in cots],
        name="product",
    )(*cots, weight)


def feature_block(core, quarter, i):
    return jnp.where(core == 0, 4 * quarter + i, 4 * i + quarter)


def arrange_body(place_ref, *refs):
    core, ring = place_ref[0], place_ref[1]
    out_ref = refs[-1]
    for k, ref in enumerate(refs[:-1]):
        quarter = (ring + 4 - k) % 4
        for i in range(4):
            out_ref[feature_block(core, quarter, i)] = ref[:, i * SPAN : (i + 1) * SPAN]


def arrange(place, quarters):
    tokens = quarters[0].shape[0]
    return pl.pallas_call(
        arrange_body,
        in_specs=[pl.BlockSpec(memory_space=pltpu.SMEM)] + [pl.BlockSpec(memory_space=pltpu.VMEM)] * 4,
        out_shape=jax.ShapeDtypeStruct((16, tokens, SPAN), bf16),
        name="arrange",
    )(place, *quarters)


def normalize_body(place_ref, own_ref, theirs_ref, mine_ref, other_ref, gain_ref, *outs, full_width):
    core, ring = place_ref[0], place_ref[1]
    means = (mine_ref[...] + other_ref[...])[:, 0:1] * (1.0 / full_width)
    scale = lax.rsqrt(means + eps)
    for k, out_ref in enumerate(outs):
        quarter = (ring + k) % 4
        for i in range(4):
            at = feature_block(core, quarter, i)
            piece = jnp.where(at // 8 == core, own_ref[at % 8].astype(f32), theirs_ref[at % 8].astype(f32))
            out_ref[:, i * SPAN : (i + 1) * SPAN] = (piece * scale * gain_ref[at]).astype(bf16)


def normalize(place, own, theirs, mine, other, gain, full_width):
    tokens = own.shape[1]
    return pl.pallas_call(
        functools.partial(normalize_body, full_width=full_width),
        in_specs=[pl.BlockSpec(memory_space=pltpu.SMEM)] + [pl.BlockSpec(memory_space=pltpu.VMEM)] * 5,
        out_shape=[jax.ShapeDtypeStruct((tokens, 4 * SPAN), bf16)] * 4,
        name="normalize",
    )(place, own, theirs, mine, other, gain.reshape(16, 1, SPAN))


def on_device(
    hash_tables, byte_table, byte_ids, hash_owner, hash_offset, gain, proj_weight, cotangent
):
    groups = lax.axis_size(AXES)
    half = lax.axis_index("mp")
    first = half == 0
    x, y, z = (lax.axis_index(axis) for axis in AXES)
    ring, side = jnp.where(first, x, y), jnp.where(first, y, x)
    _, rows, width = hash_tables.shape
    tokens = byte_ids.shape[0]
    full_width = gain.shape[0]
    cap = 2 * tokens // groups
    block = 512

    gain_half = lax.dynamic_slice_in_dim(gain, half * width, width)[None, :]
    wanted, slot = route(jnp.swapaxes(hash_owner, 1, 2), hash_offset, groups, cap)
    asked = exchange(wanted.reshape(groups, 1, LANES)).reshape(groups, LANES)

    blocks = [(proj_weight, 0)] + [(shifted(proj_weight, True, -k), k) for k in (1, 3, 2)]
    weight = joined(blocks, side, 0)
    blocks = [(weight, 0)] + [(shifted_z(weight, -k), k) for k in (2, 1, 3)]
    weight = joined(blocks, z, 1).reshape(-1, width)
    cots = [cotangent] + [shifted(cotangent, False, -k) for k in (1, 2, 3)]

    looked = lookup(asked, hash_tables, cap, block)
    fetched = exchange(looked)

    products = product(cots, weight, 256)
    quarters = [products[0]] + [shifted(products[k], False, k) for k in (1, 2, 3)]
    place = jnp.stack([half, ring]).astype(i32)
    partial = arrange(place, quarters)
    two = partial.shape[0] // 2
    other = swapped(lax.dynamic_slice_in_dim(partial, (1 - half) * two, two))
    kept = lax.dynamic_slice_in_dim(partial, half * two, two)
    dnormed = (kept.astype(f32) + other.astype(f32)).astype(bf16)
    embedded, sums = combine(slot, byte_ids, fetched, byte_table, dnormed, gain_half, block)
    others = swapped(sums)
    theirs = swapped(embedded)
    sends = dispatch(
        slot, dnormed, gain_half, embedded, sums, others, groups, cap, full_width, block
    )

    pieces = normalize(place, embedded, theirs, sums, others, gain, full_width)
    turned = [pieces[0]] + [shifted(pieces[k], False, k) for k in (1, 2, 3)]
    arrived = exchange(sends)

    projected = dot(turned[0], weight, 1, 0)
    for k in (2, 1, 3):
        piece = dot(turned[k], weight, 1, 0).astype(bf16)
        projected = projected + shifted(piece, False, -k).astype(f32)
    table_grads = accumulate(asked, arrived, rows, block)
    return (projected.astype(bf16), table_grads)


def solution(mesh):
    sides = (4, 4, 4, 2)
    torus = Mesh(mesh.devices.reshape(sides), (*AXES, "mp"))

    return jax.shard_map(
        on_device,
        mesh=torus,
        in_specs=(
            P(None, AXES, "mp"),
            P(None, "mp"),
            P(AXES),
            P(None, AXES, None),
            P(None, AXES),
            P(),
            P(AXES, "mp"),
            P(AXES, "mp"),
        ),
        out_specs=(P(AXES, "mp"), P(None, AXES, "mp")),
        check_vma=False,
    )
```

```python
import functools
import jax
import jax.numpy as jnp
from jax import lax
from jax.experimental import pallas as pl
from jax.experimental.pallas import tpu as pltpu
from jax.sharding import Mesh, PartitionSpec as P

eps = 1e-05
f32, bf16, i32 = jnp.float32, jnp.bfloat16, jnp.int32
LANES = 128
SPAN = 256
AXES = ("x", "y", "z")


def iota(shape, dim):
    return lax.broadcasted_iota(i32, shape, dim)


def dot(a, b, ca, cb):
    return lax.dot_general(a, b, (((ca,), (cb,)), ((), ())), preferred_element_type=f32)


def route_body(owner_ref, offset_ref, wanted_ref, slot_ref, *, groups, cap):
    ngram, _, tokens = owner_ref.shape
    earlier = (iota((tokens, tokens), 0) < iota((tokens, tokens), 1)).astype(f32).astype(bf16)
    lane = iota((groups, LANES), 1)
    wanted = jnp.full((groups, LANES), -1, i32)
    for k in range(ngram):
        owner = owner_ref[k]
        offset = offset_ref[k : k + 1, :]
        mine = jnp.broadcast_to(owner, (groups, tokens)) == iota((groups, tokens), 0)
        before = dot(mine.astype(f32).astype(bf16), earlier, 1, 0).astype(i32)
        rank = jnp.sum(jnp.where(mine, before, 0), axis=0, keepdims=True)
        slot_ref[k : k + 1, :] = owner * (ngram * cap) + k * cap + rank
        for r in range(cap):
            hit = jnp.where(mine & (before == r), offset + 1, 0)
            value = jnp.sum(hit, axis=1, keepdims=True) - 1
            wanted = jnp.where(lane == k * cap + r, value, wanted)
    wanted_ref[...] = wanted


def route(owner, offset, groups, cap):
    ngram, _, tokens = owner.shape
    return pl.pallas_call(
        functools.partial(route_body, groups=groups, cap=cap),
        out_shape=(
            jax.ShapeDtypeStruct((groups, LANES), i32),
            jax.ShapeDtypeStruct((ngram, tokens), i32),
        ),
        name="route",
    )(owner, offset)


def row_picks(asked, k, cap, rows):
    groups = asked.shape[0]
    total = groups * cap
    spread = (iota((total, groups), 0) // cap == iota((total, groups), 1)).astype(f32).astype(bf16)
    code = asked + 1
    high = (code >> 5).astype(f32).astype(bf16)
    low = (code & 31).astype(f32).astype(bf16)
    codes = dot(spread, high, 1, 0) * 32.0 + dot(spread, low, 1, 0)
    place = iota((total, LANES), 1) == k * cap + iota((total, LANES), 0) % cap
    column = jnp.sum(jnp.where(place, codes, 0.0), axis=1, keepdims=True).astype(i32) - 1
    return (column == iota((total, rows), 1)).astype(f32).astype(bf16)


def lookup_body(asked_ref, table_ref, out_ref, picks_ref, *, cap):
    k = pl.program_id(0)
    rows = table_ref.shape[1]

    @pl.when(pl.program_id(1) == 0)
    def _():
        picks_ref[...] = row_picks(asked_ref[...], k, cap, rows)

    out = dot(picks_ref[...], table_ref[0], 1, 0).astype(bf16)
    out_ref[...] = out.reshape(out_ref.shape)


def lookup(asked, tables, cap, block):
    groups = asked.shape[0]
    ngram, rows, width = tables.shape
    return pl.pallas_call(
        functools.partial(lookup_body, cap=cap),
        grid=(ngram, width // block),
        in_specs=[
            pl.BlockSpec((groups, LANES), lambda k, j: (0, 0)),
            pl.BlockSpec((1, rows, block), lambda k, j: (k, 0, j)),
        ],
        out_specs=pl.BlockSpec((groups, 1, cap, block), lambda k, j: (0, k, 0, j)),
        out_shape=jax.ShapeDtypeStruct((groups, ngram, cap, width), bf16),
        scratch_shapes=[pltpu.VMEM((groups * cap, rows), bf16)],
        name="lookup",
    )(asked, tables)


def slot_columns(slot_ref, slots):
    ngram, tokens = slot_ref.shape
    filled = jnp.concatenate([slot_ref[...], jnp.zeros((8 - ngram, tokens), i32)], axis=0)
    columns = filled.astype(f32).T.astype(i32)
    place = iota((tokens, slots), 1)
    hit = place == columns[:, 0:1]
    for k in range(1, ngram):
        hit = hit | (place == columns[:, k : k + 1])
    return hit.astype(f32).astype(bf16)


def side_by_side(ref):
    return jnp.concatenate([ref[i] for i in range(ref.shape[0])], axis=1)


def combine_body(
    slot_ref, ids_ref, fetched_ref, bytes_ref, out_ref, square_ref, picks_ref, codes_ref
):
    tokens, slots = picks_ref.shape

    @pl.when(pl.program_id(0) == 0)
    def _():
        picks_ref[...] = slot_columns(slot_ref, slots)
        vocab = codes_ref.shape[0]
        codes_ref[...] = (iota((vocab, tokens), 0) == ids_ref[...]).astype(f32).astype(bf16)
        square_ref[...] = jnp.zeros(square_ref.shape, f32)

    block = fetched_ref.shape[-1]
    fetched = fetched_ref[...].reshape(slots, block)
    summed = dot(picks_ref[...], fetched, 1, 0) + dot(codes_ref[...], bytes_ref[...], 0, 0)
    embedded = summed.astype(bf16)
    for i in range(block // SPAN):
        out_ref[i] = embedded[:, i * SPAN : (i + 1) * SPAN]
    values = embedded.astype(f32)
    square_ref[...] += jnp.sum(values * values, axis=1, keepdims=True)


def combine(slot, ids, fetched, byte_table, block):
    groups, ngram, cap, width = fetched.shape
    tokens = slot.shape[1]
    vocab = byte_table.shape[0]
    slots = groups * ngram * cap
    return pl.pallas_call(
        combine_body,
        grid=(width // block,),
        in_specs=[
            pl.BlockSpec((ngram, tokens), lambda j: (0, 0)),
            pl.BlockSpec((1, tokens), lambda j: (0, 0)),
            pl.BlockSpec((groups, ngram, cap, block), lambda j: (0, 0, 0, j)),
            pl.BlockSpec((vocab, block), lambda j: (0, j)),
        ],
        out_specs=(
            pl.BlockSpec((block // SPAN, tokens, SPAN), lambda j: (j, 0, 0)),
            pl.BlockSpec((tokens, LANES), lambda j: (0, 0)),
        ),
        out_shape=(
            jax.ShapeDtypeStruct((width // SPAN, tokens, SPAN), bf16),
            jax.ShapeDtypeStruct((tokens, LANES), f32),
        ),
        scratch_shapes=[pltpu.VMEM((tokens, slots), bf16), pltpu.VMEM((vocab, tokens), bf16)],
        name="combine",
    )(slot, ids.reshape(1, tokens), fetched, byte_table)


def dispatch_body(
    slot_ref, kept_ref, other_ref, gain_ref, embedded_ref, sq0_ref, sq1_ref, in0_ref, in1_ref, out_ref, picks_ref, *, full_width
):
    slots, tokens = picks_ref.shape

    @pl.when(pl.program_id(0) == 0)
    def _():
        place = iota((slots, tokens), 0)
        hit = place == slot_ref[0:1, :]
        for k in range(1, slot_ref.shape[0]):
            hit = hit | (place == slot_ref[k : k + 1, :])
        picks_ref[...] = hit.astype(f32).astype(bf16)

    scale = lax.rsqrt((sq0_ref[...] + sq1_ref[...])[:, 0:1] * (1.0 / full_width) + eps)
    inner = (in0_ref[...] + in1_ref[...])[:, 0:1] * (1.0 / full_width)
    values = side_by_side(embedded_ref).astype(f32)
    dnormed = side_by_side(kept_ref).astype(f32) + side_by_side(other_ref).astype(f32)
    scaled = dnormed * gain_ref[...]
    dembed = scale * scaled - values * (scale * scale * scale * inner)
    out = dot(picks_ref[...], dembed.astype(bf16), 1, 0).astype(bf16)
    out_ref[...] = out.reshape(out_ref.shape)


def dispatch(slot, kept, other, gain, embedded, sums, groups, cap, full_width, block):
    ngram, tokens = slot.shape
    width = embedded.shape[0] * SPAN
    slots = groups * ngram * cap
    blocked = pl.BlockSpec((block // SPAN, tokens, SPAN), lambda j: (j, 0, 0))
    total = pl.BlockSpec((tokens, LANES), lambda j: (0, 0))
    return pl.pallas_call(
        functools.partial(dispatch_body, full_width=full_width),
        grid=(width // block,),
        in_specs=[
            pl.BlockSpec((ngram, tokens), lambda j: (0, 0)),
            blocked,
            blocked,
            pl.BlockSpec((1, block), lambda j: (0, j)),
            blocked,
            total,
            total,
            total,
            total,
        ],
        out_specs=pl.BlockSpec((groups, ngram, cap, block), lambda j: (0, 0, 0, j)),
        out_shape=jax.ShapeDtypeStruct((groups, ngram, cap, width), bf16),
        scratch_shapes=[pltpu.VMEM((slots, tokens), bf16)],
        name="dispatch",
    )(slot, kept, other, gain, embedded, *sums)


def accumulate_body(asked_ref, arrived_ref, out_ref, picks_ref, *, cap):
    k = pl.program_id(0)
    rows = out_ref.shape[1]
    groups = asked_ref.shape[0]
    total = groups * cap

    @pl.when(pl.program_id(1) == 0)
    def _():
        spread = (iota((total, groups), 0) // cap == iota((total, groups), 1)).astype(f32).astype(bf16)
        code = asked_ref[...] + 1
        high = (code >> 5).astype(f32).astype(bf16)
        low = (code & 31).astype(f32).astype(bf16)
        codes = dot(high, spread, 0, 1) * 32.0 + dot(low, spread, 0, 1)
        place = iota((LANES, total), 0) == k * cap + iota((LANES, total), 1) % cap
        line = jnp.sum(jnp.where(place, codes, 0.0), axis=0, keepdims=True).astype(i32) - 1
        picks_ref[...] = (iota((rows, total), 0) == line).astype(f32).astype(bf16)

    arrived = arrived_ref[...].reshape(total, arrived_ref.shape[-1])
    out_ref[0] = dot(picks_ref[...], arrived, 1, 0).astype(bf16)


def accumulate(asked, arrived, rows, block):
    groups, ngram, cap, width = arrived.shape
    return pl.pallas_call(
        functools.partial(accumulate_body, cap=cap),
        grid=(ngram, width // block),
        in_specs=[
            pl.BlockSpec((groups, LANES), lambda k, j: (0, 0)),
            pl.BlockSpec((groups, 1, cap, block), lambda k, j: (0, k, 0, j)),
        ],
        out_specs=pl.BlockSpec((1, rows, block), lambda k, j: (k, 0, j)),
        out_shape=jax.ShapeDtypeStruct((ngram, rows, width), bf16),
        scratch_shapes=[pltpu.VMEM((rows, groups * cap), bf16)],
        name="accumulate",
    )(asked, arrived)


def exchange(array):
    return lax.all_to_all(array, AXES, split_axis=0, concat_axis=0, tiled=True)


def swapped(array):
    return lax.ppermute(array, "mp", [(0, 1), (1, 0)])


def shifted(array, turned, by):
    pairs = []
    for x in range(4):
        for y in range(4):
            for c in range(2):
                along_x = (c == 0) != turned
                to = ((x + by) % 4, y) if along_x else (x, (y + by) % 4)
                pairs.append(((x * 4 + y) * 2 + c, (to[0] * 4 + to[1]) * 2 + c))
    return lax.ppermute(array, ("x", "y", "mp"), pairs)


def shifted_z(array, by):
    return lax.ppermute(array, "z", [(i, (i + by) % 4) for i in range(4)])


def joined(blocks, here, dim):
    shape = list(blocks[0][0].shape)
    shape.insert(dim, 4)
    whole = jnp.zeros(shape, blocks[0][0].dtype)
    for block, away in blocks:
        whole = lax.dynamic_update_slice_in_dim(
            whole, jnp.expand_dims(block, dim), (here + away) % 4, dim
        )
    return whole


def product_body(*refs):
    cots, weight_ref, outs = refs[:4], refs[4], refs[5:]
    for cot_ref, out_ref in zip(cots, outs, strict=True):
        out_ref[...] = dot(cot_ref[...], weight_ref[...], 1, 1).astype(bf16)


def product(cots, weight, block):
    tokens, width = cots[0].shape
    rows = weight.shape[0]
    return pl.pallas_call(
        product_body,
        grid=(rows // block,),
        in_specs=[pl.BlockSpec((tokens, width), lambda j: (0, 0)) for _ in cots]
        + [pl.BlockSpec((block, width), lambda j: (j, 0))],
        out_specs=[pl.BlockSpec((tokens, block), lambda j: (0, j)) for _ in cots],
        out_shape=[jax.ShapeDtypeStruct((tokens, rows), bf16) for _ in cots],
        name="product",
    )(*cots, weight)


def forward_body(*refs):
    pieces, weight_ref, outs = refs[:4], refs[4], refs[5:]
    for piece_ref, out_ref in zip(pieces, outs, strict=True):
        out_ref[...] = dot(piece_ref[...], weight_ref[...], 1, 0).astype(out_ref.dtype)


def forward(pieces, weight, block):
    tokens, rows = pieces[0].shape
    width = weight.shape[1]
    return pl.pallas_call(
        forward_body,
        grid=(width // block,),
        in_specs=[pl.BlockSpec((tokens, rows), lambda j: (0, 0)) for _ in pieces]
        + [pl.BlockSpec((rows, block), lambda j: (0, j))],
        out_specs=[pl.BlockSpec((tokens, block), lambda j: (0, j)) for _ in pieces],
        out_shape=[
            jax.ShapeDtypeStruct((tokens, width), bf16 if k else f32) for k in range(len(pieces))
        ],
        name="forward",
    )(*pieces, weight)


def feature_block(core, quarter, i):
    return jnp.where(core == 0, 4 * quarter + i, 4 * i + quarter)


def arrange_body(place_ref, own_ref, theirs_ref, gain_ref, *refs):
    core, ring = place_ref[0], place_ref[1]
    quarters, (kept_ref, given_ref, inner_ref) = refs[:-3], refs[-3:]
    tokens = inner_ref.shape[0]
    total = jnp.zeros((tokens, SPAN), f32)
    for k, ref in enumerate(quarters):
        quarter = (ring + 4 - k) % 4
        for i in range(4):
            at = feature_block(core, quarter, i)
            here, ours = at % 8, at // 8 == core
            piece = ref[:, i * SPAN : (i + 1) * SPAN]
            values = jnp.where(ours, own_ref[here].astype(f32), theirs_ref[here].astype(f32))
            total += values * (piece.astype(f32) * gain_ref[at])

            @pl.when(ours)
            def _():
                kept_ref[here] = piece

            @pl.when(jnp.logical_not(ours))
            def _():
                given_ref[here] = piece

    inner_ref[...] = jnp.broadcast_to(jnp.sum(total, axis=1, keepdims=True), inner_ref.shape)


def arrange(place, own, theirs, gain, quarters):
    tokens = quarters[0].shape[0]
    half = jax.ShapeDtypeStruct((8, tokens, SPAN), bf16)
    return pl.pallas_call(
        arrange_body,
        in_specs=[pl.BlockSpec(memory_space=pltpu.SMEM)] + [pl.BlockSpec(memory_space=pltpu.VMEM)] * 7,
        out_shape=(half, half, jax.ShapeDtypeStruct((tokens, LANES), f32)),
        name="arrange",
    )(place, own, theirs, gain.reshape(16, 1, SPAN), *quarters)


def normalize_body(place_ref, own_ref, theirs_ref, mine_ref, other_ref, gain_ref, *outs, full_width):
    core, ring = place_ref[0], place_ref[1]
    means = (mine_ref[...] + other_ref[...])[:, 0:1] * (1.0 / full_width)
    scale = lax.rsqrt(means + eps)
    for k, out_ref in enumerate(outs):
        quarter = (ring + k) % 4
        for i in range(4):
            at = feature_block(core, quarter, i)
            piece = jnp.where(at // 8 == core, own_ref[at % 8].astype(f32), theirs_ref[at % 8].astype(f32))
            out_ref[:, i * SPAN : (i + 1) * SPAN] = (piece * scale * gain_ref[at]).astype(bf16)


def normalize(place, own, theirs, mine, other, gain, full_width):
    tokens = own.shape[1]
    return pl.pallas_call(
        functools.partial(normalize_body, full_width=full_width),
        in_specs=[pl.BlockSpec(memory_space=pltpu.SMEM)] + [pl.BlockSpec(memory_space=pltpu.VMEM)] * 5,
        out_shape=[jax.ShapeDtypeStruct((tokens, 4 * SPAN), bf16)] * 4,
        name="normalize",
    )(place, own, theirs, mine, other, gain.reshape(16, 1, SPAN))


def on_device(
    hash_tables, byte_table, byte_ids, hash_owner, hash_offset, gain, proj_weight, cotangent
):
    groups = lax.axis_size(AXES)
    half = lax.axis_index("mp")
    first = half == 0
    x, y, z = (lax.axis_index(axis) for axis in AXES)
    ring, side = jnp.where(first, x, y), jnp.where(first, y, x)
    _, rows, width = hash_tables.shape
    tokens = byte_ids.shape[0]
    full_width = gain.shape[0]
    cap = 2 * tokens // groups
    block = 512

    gain_half = lax.dynamic_slice_in_dim(gain, half * width, width)[None, :]
    wanted, slot = route(jnp.swapaxes(hash_owner, 1, 2), hash_offset, groups, cap)
    asked = exchange(wanted.reshape(groups, 1, LANES)).reshape(groups, LANES)

    blocks = [(proj_weight, 0)] + [(shifted(proj_weight, True, -k), k) for k in (1, 3, 2)]
    weight = joined(blocks, side, 0)
    after, before = shifted_z(weight, -1), shifted_z(weight, 1)
    opposite = [shifted_z(after[:2], -1), shifted_z(before[2:], 1)]
    blocks = [(weight, 0), (after, 1), (before, 3), (jnp.concatenate(opposite), 2)]
    weight = joined(blocks, z, 1).reshape(-1, width)
    two, one, three = (shifted(cotangent, False, -k) for k in (2, 1, 3))
    cots = [cotangent, one, two, three]

    looked = lookup(asked, hash_tables, cap, 2 * block)
    fetched = exchange(looked)

    products = product(cots, weight, 256)
    quarters = [products[0]] + [shifted(products[k], False, k) for k in (1, 2, 3)]
    place = jnp.stack([half, ring]).astype(i32)
    embedded, square = combine(slot, byte_ids, fetched, byte_table, block)
    squares = (square, swapped(square))
    theirs = swapped(embedded)
    pieces = normalize(place, embedded, theirs, *squares, gain, full_width)
    turned = [pieces[0]] + [shifted(pieces[k], False, k) for k in (1, 2, 3)]
    kept, given, inner = arrange(place, embedded, theirs, gain, quarters)
    other = swapped(given)
    sums = (*squares, inner, swapped(inner))
    sends = dispatch(slot, kept, other, gain_half, embedded, sums, groups, cap, full_width, block)
    arrived = exchange(sends)

    projected, *others = forward(turned, weight, block)
    for k in (2, 1, 3):
        projected = projected + shifted(others[k - 1], False, -k).astype(f32)
    table_grads = accumulate(asked, arrived, rows, 2 * block)
    return (projected.astype(bf16), table_grads)


def solution(mesh):
    sides = (4, 4, 4, 2)
    torus = Mesh(mesh.devices.reshape(sides), (*AXES, "mp"))

    return jax.shard_map(
        on_device,
        mesh=torus,
        in_specs=(
            P(None, AXES, "mp"),
            P(None, "mp"),
            P(AXES),
            P(None, AXES, None),
            P(None, AXES),
            P(),
            P(AXES, "mp"),
            P(AXES, "mp"),
        ),
        out_specs=(P(AXES, "mp"), P(None, AXES, "mp")),
        check_vma=False,
    )
```

```python
import functools
import jax
import jax.numpy as jnp
from jax import lax
from jax.experimental import pallas as pl
from jax.experimental.pallas import tpu as pltpu
from jax.sharding import Mesh, PartitionSpec as P

eps = 1e-05
f32, bf16, i32 = jnp.float32, jnp.bfloat16, jnp.int32
LANES = 128
SPAN = 256
AXES = ("x", "y", "z")


def iota(shape, dim):
    return lax.broadcasted_iota(i32, shape, dim)


def dot(a, b, ca, cb):
    return lax.dot_general(a, b, (((ca,), (cb,)), ((), ())), preferred_element_type=f32)


def route_body(owner_ref, offset_ref, wanted_ref, slot_ref, *, groups, cap):
    ngram, _, tokens = owner_ref.shape
    earlier = (iota((tokens, tokens), 0) < iota((tokens, tokens), 1)).astype(f32).astype(bf16)
    lane = iota((groups, LANES), 1)
    wanted = jnp.full((groups, LANES), -1, i32)
    for k in range(ngram):
        owner = owner_ref[k]
        offset = offset_ref[k : k + 1, :]
        mine = jnp.broadcast_to(owner, (groups, tokens)) == iota((groups, tokens), 0)
        before = dot(mine.astype(f32).astype(bf16), earlier, 1, 0).astype(i32)
        rank = jnp.sum(jnp.where(mine, before, 0), axis=0, keepdims=True)
        slot_ref[k : k + 1, :] = owner * (ngram * cap) + k * cap + rank
        for r in range(cap):
            hit = jnp.where(mine & (before == r), offset + 1, 0)
            value = jnp.sum(hit, axis=1, keepdims=True) - 1
            wanted = jnp.where(lane == k * cap + r, value, wanted)
    wanted_ref[...] = wanted


def route(owner, offset, groups, cap):
    ngram, _, tokens = owner.shape
    return pl.pallas_call(
        functools.partial(route_body, groups=groups, cap=cap),
        out_shape=(
            jax.ShapeDtypeStruct((groups, LANES), i32),
            jax.ShapeDtypeStruct((ngram, tokens), i32),
        ),
        name="route",
    )(owner, offset)


def row_picks(asked, k, cap, rows):
    groups = asked.shape[0]
    total = groups * cap
    spread = (iota((total, groups), 0) // cap == iota((total, groups), 1)).astype(f32).astype(bf16)
    code = asked + 1
    high = (code >> 5).astype(f32).astype(bf16)
    low = (code & 31).astype(f32).astype(bf16)
    codes = dot(spread, high, 1, 0) * 32.0 + dot(spread, low, 1, 0)
    place = iota((total, LANES), 1) == k * cap + iota((total, LANES), 0) % cap
    column = jnp.sum(jnp.where(place, codes, 0.0), axis=1, keepdims=True).astype(i32) - 1
    return (column == iota((total, rows), 1)).astype(f32).astype(bf16)


def lookup_body(asked_ref, table_ref, out_ref, picks_ref, *, cap):
    k = pl.program_id(0)
    rows = table_ref.shape[1]

    @pl.when(pl.program_id(1) == 0)
    def _():
        picks_ref[...] = row_picks(asked_ref[...], k, cap, rows)

    out = dot(picks_ref[...], table_ref[0], 1, 0).astype(bf16)
    out_ref[...] = out.reshape(out_ref.shape)


def lookup(asked, tables, cap, block):
    groups = asked.shape[0]
    ngram, rows, width = tables.shape
    return pl.pallas_call(
        functools.partial(lookup_body, cap=cap),
        grid=(ngram, width // block),
        in_specs=[
            pl.BlockSpec((groups, LANES), lambda k, j: (0, 0)),
            pl.BlockSpec((1, rows, block), lambda k, j: (k, 0, j)),
        ],
        out_specs=pl.BlockSpec((groups, 1, cap, block), lambda k, j: (0, k, 0, j)),
        out_shape=jax.ShapeDtypeStruct((groups, ngram, cap, width), bf16),
        scratch_shapes=[pltpu.VMEM((groups * cap, rows), bf16)],
        name="lookup",
    )(asked, tables)


def slot_columns(slot_ref, slots):
    ngram, tokens = slot_ref.shape
    filled = jnp.concatenate([slot_ref[...], jnp.zeros((8 - ngram, tokens), i32)], axis=0)
    columns = filled.astype(f32).T.astype(i32)
    place = iota((tokens, slots), 1)
    hit = place == columns[:, 0:1]
    for k in range(1, ngram):
        hit = hit | (place == columns[:, k : k + 1])
    return hit.astype(f32).astype(bf16)


def side_by_side(ref):
    return jnp.concatenate([ref[i] for i in range(ref.shape[0])], axis=1)


def combine_body(
    slot_ref, ids_ref, fetched_ref, bytes_ref, out_ref, square_ref, picks_ref, codes_ref
):
    tokens, slots = picks_ref.shape

    @pl.when(pl.program_id(0) == 0)
    def _():
        picks_ref[...] = slot_columns(slot_ref, slots)
        vocab = codes_ref.shape[0]
        codes_ref[...] = (iota((vocab, tokens), 0) == ids_ref[...]).astype(f32).astype(bf16)
        square_ref[...] = jnp.zeros(square_ref.shape, f32)

    block = fetched_ref.shape[-1]
    fetched = fetched_ref[...].reshape(slots, block)
    summed = dot(picks_ref[...], fetched, 1, 0) + dot(codes_ref[...], bytes_ref[...], 0, 0)
    embedded = summed.astype(bf16)
    for i in range(block // SPAN):
        out_ref[i] = embedded[:, i * SPAN : (i + 1) * SPAN]
    values = embedded.astype(f32)
    square_ref[...] += jnp.sum(values * values, axis=1, keepdims=True)


def combine(slot, ids, fetched, byte_table, block):
    groups, ngram, cap, width = fetched.shape
    tokens = slot.shape[1]
    vocab = byte_table.shape[0]
    slots = groups * ngram * cap
    return pl.pallas_call(
        combine_body,
        grid=(width // block,),
        in_specs=[
            pl.BlockSpec((ngram, tokens), lambda j: (0, 0)),
            pl.BlockSpec((1, tokens), lambda j: (0, 0)),
            pl.BlockSpec((groups, ngram, cap, block), lambda j: (0, 0, 0, j)),
            pl.BlockSpec((vocab, block), lambda j: (0, j)),
        ],
        out_specs=(
            pl.BlockSpec((block // SPAN, tokens, SPAN), lambda j: (j, 0, 0)),
            pl.BlockSpec((tokens, LANES), lambda j: (0, 0)),
        ),
        out_shape=(
            jax.ShapeDtypeStruct((width // SPAN, tokens, SPAN), bf16),
            jax.ShapeDtypeStruct((tokens, LANES), f32),
        ),
        scratch_shapes=[pltpu.VMEM((tokens, slots), bf16), pltpu.VMEM((vocab, tokens), bf16)],
        name="combine",
    )(slot, ids.reshape(1, tokens), fetched, byte_table)


def dispatch_body(
    slot_ref, kept_ref, other_ref, gain_ref, embedded_ref, sq0_ref, sq1_ref, in0_ref, in1_ref, out_ref, picks_ref, *, full_width
):
    slots, tokens = picks_ref.shape

    @pl.when(pl.program_id(0) == 0)
    def _():
        place = iota((slots, tokens), 0)
        hit = place == slot_ref[0:1, :]
        for k in range(1, slot_ref.shape[0]):
            hit = hit | (place == slot_ref[k : k + 1, :])
        picks_ref[...] = hit.astype(f32).astype(bf16)

    scale = lax.rsqrt((sq0_ref[...] + sq1_ref[...])[:, 0:1] * (1.0 / full_width) + eps)
    inner = (in0_ref[...] + in1_ref[...])[:, 0:1] * (1.0 / full_width)
    values = side_by_side(embedded_ref).astype(f32)
    dnormed = side_by_side(kept_ref).astype(f32) + side_by_side(other_ref).astype(f32)
    scaled = dnormed * gain_ref[...]
    dembed = scale * scaled - values * (scale * scale * scale * inner)
    out = dot(picks_ref[...], dembed.astype(bf16), 1, 0).astype(bf16)
    out_ref[...] = out.reshape(out_ref.shape)


def dispatch(slot, kept, other, gain, embedded, sums, groups, cap, full_width, block):
    ngram, tokens = slot.shape
    width = embedded.shape[0] * SPAN
    slots = groups * ngram * cap
    blocked = pl.BlockSpec((block // SPAN, tokens, SPAN), lambda j: (j, 0, 0))
    total = pl.BlockSpec((tokens, LANES), lambda j: (0, 0))
    return pl.pallas_call(
        functools.partial(dispatch_body, full_width=full_width),
        grid=(width // block,),
        in_specs=[
            pl.BlockSpec((ngram, tokens), lambda j: (0, 0)),
            blocked,
            blocked,
            pl.BlockSpec((1, block), lambda j: (0, j)),
            blocked,
            total,
            total,
            total,
            total,
        ],
        out_specs=pl.BlockSpec((groups, ngram, cap, block), lambda j: (0, 0, 0, j)),
        out_shape=jax.ShapeDtypeStruct((groups, ngram, cap, width), bf16),
        scratch_shapes=[pltpu.VMEM((slots, tokens), bf16)],
        name="dispatch",
    )(slot, kept, other, gain, embedded, *sums)


def accumulate_body(asked_ref, arrived_ref, out_ref, picks_ref, *, cap):
    k = pl.program_id(0)
    rows = out_ref.shape[1]
    groups = asked_ref.shape[0]
    total = groups * cap

    @pl.when(pl.program_id(1) == 0)
    def _():
        spread = (iota((total, groups), 0) // cap == iota((total, groups), 1)).astype(f32).astype(bf16)
        code = asked_ref[...] + 1
        high = (code >> 5).astype(f32).astype(bf16)
        low = (code & 31).astype(f32).astype(bf16)
        codes = dot(high, spread, 0, 1) * 32.0 + dot(low, spread, 0, 1)
        place = iota((LANES, total), 0) == k * cap + iota((LANES, total), 1) % cap
        line = jnp.sum(jnp.where(place, codes, 0.0), axis=0, keepdims=True).astype(i32) - 1
        picks_ref[...] = (iota((rows, total), 0) == line).astype(f32).astype(bf16)

    arrived = arrived_ref[...].reshape(total, arrived_ref.shape[-1])
    out_ref[0] = dot(picks_ref[...], arrived, 1, 0).astype(bf16)


def accumulate(asked, arrived, rows, block):
    groups, ngram, cap, width = arrived.shape
    return pl.pallas_call(
        functools.partial(accumulate_body, cap=cap),
        grid=(ngram, width // block),
        in_specs=[
            pl.BlockSpec((groups, LANES), lambda k, j: (0, 0)),
            pl.BlockSpec((groups, 1, cap, block), lambda k, j: (0, k, 0, j)),
        ],
        out_specs=pl.BlockSpec((1, rows, block), lambda k, j: (k, 0, j)),
        out_shape=jax.ShapeDtypeStruct((ngram, rows, width), bf16),
        scratch_shapes=[pltpu.VMEM((rows, groups * cap), bf16)],
        name="accumulate",
    )(asked, arrived)


def exchange(array):
    return lax.all_to_all(array, AXES, split_axis=0, concat_axis=0, tiled=True)


def swapped(array):
    return lax.ppermute(array, "mp", [(0, 1), (1, 0)])


def shifted(array, turned, by):
    pairs = []
    for x in range(4):
        for y in range(4):
            for c in range(2):
                along_x = (c == 0) != turned
                to = ((x + by) % 4, y) if along_x else (x, (y + by) % 4)
                pairs.append(((x * 4 + y) * 2 + c, (to[0] * 4 + to[1]) * 2 + c))
    return lax.ppermute(array, ("x", "y", "mp"), pairs)


def shifted_z(array, by):
    return lax.ppermute(array, "z", [(i, (i + by) % 4) for i in range(4)])


def joined(blocks, here, dim):
    shape = list(blocks[0][0].shape)
    shape.insert(dim, 4)
    whole = jnp.zeros(shape, blocks[0][0].dtype)
    for block, away in blocks:
        whole = lax.dynamic_update_slice_in_dim(
            whole, jnp.expand_dims(block, dim), (here + away) % 4, dim
        )
    return whole


def product_body(*refs):
    cots, weight_ref, outs = refs[:4], refs[4], refs[5:]
    for cot_ref, out_ref in zip(cots, outs, strict=True):
        out_ref[...] = dot(cot_ref[...], weight_ref[...], 1, 1).astype(bf16)


def product(cots, weight, block):
    tokens, width = cots[0].shape
    rows = weight.shape[0]
    return pl.pallas_call(
        product_body,
        grid=(rows // block,),
        in_specs=[pl.BlockSpec((tokens, width), lambda j: (0, 0)) for _ in cots]
        + [pl.BlockSpec((block, width), lambda j: (j, 0))],
        out_specs=[pl.BlockSpec((tokens, block), lambda j: (0, j)) for _ in cots],
        out_shape=[jax.ShapeDtypeStruct((tokens, rows), bf16) for _ in cots],
        name="product",
    )(*cots, weight)


def forward_body(*refs):
    count = len(refs) // 2
    pieces, weight_ref, outs = refs[:count], refs[count], refs[count + 1 :]
    for piece_ref, out_ref in zip(pieces, outs, strict=True):
        out_ref[...] = dot(piece_ref[...], weight_ref[...], 1, 0).astype(out_ref.dtype)


def forward(pieces, weight, block, types):
    tokens, rows = pieces[0].shape
    width = weight.shape[1]
    return pl.pallas_call(
        forward_body,
        grid=(width // block,),
        in_specs=[pl.BlockSpec((tokens, rows), lambda j: (0, 0)) for _ in pieces]
        + [pl.BlockSpec((rows, block), lambda j: (0, j))],
        out_specs=[pl.BlockSpec((tokens, block), lambda j: (0, j)) for _ in pieces],
        out_shape=[jax.ShapeDtypeStruct((tokens, width), kind) for kind in types],
        name="forward",
    )(*pieces, weight)


def feature_block(core, quarter, i):
    return jnp.where(core == 0, 4 * quarter + i, 4 * i + quarter)


def settle_body(place_ref, own_ref, theirs_ref, gain_ref, mine_ref, other_ref, *refs, full_width):
    core, ring = place_ref[0], place_ref[1]
    quarters, (kept_ref, given_ref, inner_ref), pieces = refs[:4], refs[4:7], refs[7:]
    tokens = inner_ref.shape[0]
    scale = lax.rsqrt((mine_ref[...] + other_ref[...])[:, 0:1] * (1.0 / full_width) + eps)
    total = jnp.zeros((tokens, SPAN), f32)
    for k, ref in enumerate(quarters):
        quarter = (ring + 4 - k) % 4
        for i in range(4):
            at = feature_block(core, quarter, i)
            here, ours = at % 8, at // 8 == core
            lanes = slice(i * SPAN, (i + 1) * SPAN)
            piece = ref[:, lanes]
            gain = gain_ref[at]
            values = jnp.where(ours, own_ref[here].astype(f32), theirs_ref[here].astype(f32))
            total += values * (piece.astype(f32) * gain)
            pieces[(4 - k) % 4][:, lanes] = (values * scale * gain).astype(bf16)

            @pl.when(ours)
            def _():
                kept_ref[here] = piece

            @pl.when(jnp.logical_not(ours))
            def _():
                given_ref[here] = piece

    inner_ref[...] = jnp.broadcast_to(jnp.sum(total, axis=1, keepdims=True), inner_ref.shape)


def settle(place, own, theirs, gain, squares, quarters, full_width, block):
    tokens = own.shape[1]
    blocked = pl.BlockSpec((8, block, SPAN), lambda j: (0, j, 0))
    flat = pl.BlockSpec((block, 4 * SPAN), lambda j: (j, 0))
    total = pl.BlockSpec((block, LANES), lambda j: (j, 0))
    half = jax.ShapeDtypeStruct((8, tokens, SPAN), bf16)
    out = pl.pallas_call(
        functools.partial(settle_body, full_width=full_width),
        grid=(tokens // block,),
        in_specs=[
            pl.BlockSpec(memory_space=pltpu.SMEM),
            blocked,
            blocked,
            pl.BlockSpec((16, 1, SPAN), lambda j: (0, 0, 0)),
            total,
            total,
            *[flat] * 4,
        ],
        out_specs=[blocked, blocked, total, *[flat] * 4],
        out_shape=[
            half,
            half,
            jax.ShapeDtypeStruct((tokens, LANES), f32),
            *[jax.ShapeDtypeStruct((tokens, 4 * SPAN), bf16)] * 4,
        ],
        name="settle",
    )(place, own, theirs, gain.reshape(16, 1, SPAN), *squares, *quarters)
    return out[0], out[1], out[2], out[3:]


def on_device(
    hash_tables, byte_table, byte_ids, hash_owner, hash_offset, gain, proj_weight, cotangent
):
    groups = lax.axis_size(AXES)
    half = lax.axis_index("mp")
    first = half == 0
    x, y, z = (lax.axis_index(axis) for axis in AXES)
    ring, side = jnp.where(first, x, y), jnp.where(first, y, x)
    _, rows, width = hash_tables.shape
    tokens = byte_ids.shape[0]
    full_width = gain.shape[0]
    cap = 2 * tokens // groups
    block = 512

    gain_half = lax.dynamic_slice_in_dim(gain, half * width, width)[None, :]
    wanted, slot = route(jnp.swapaxes(hash_owner, 1, 2), hash_offset, groups, cap)
    asked = exchange(wanted.reshape(groups, 1, LANES)).reshape(groups, LANES)

    blocks = [(proj_weight, 0)] + [(shifted(proj_weight, True, -k), k) for k in (1, 3, 2)]
    weight = joined(blocks, side, 0)
    after, before = shifted_z(weight, -1), shifted_z(weight, 1)
    opposite = [shifted_z(after[:2], -1), shifted_z(before[2:], 1)]
    blocks = [(weight, 0), (after, 1), (before, 3), (jnp.concatenate(opposite), 2)]
    weight = joined(blocks, z, 1).reshape(-1, width)
    two, one, three = (shifted(cotangent, False, -k) for k in (2, 1, 3))
    cots = [cotangent, one, two, three]

    looked = lookup(asked, hash_tables, cap, 2 * block)
    fetched = exchange(looked)

    products = product(cots, weight, 256)
    quarters = [products[0]] + [shifted(products[k], False, k) for k in (1, 2, 3)]
    place = jnp.stack([half, ring]).astype(i32)
    embedded, square = combine(slot, byte_ids, fetched, byte_table, block)
    squares = (square, swapped(square))
    theirs = swapped(embedded)
    kept, given, inner, pieces = settle(
        place, embedded, theirs, gain, squares, quarters, full_width, tokens // 4
    )
    other = swapped(given)
    sums = (*squares, inner, swapped(inner))
    across, near, last = (shifted(pieces[k], False, k) for k in (2, 1, 3))
    sends = dispatch(slot, kept, other, gain_half, embedded, sums, groups, cap, full_width, block)
    arrived = exchange(sends)

    returned = [shifted(forward([across], weight, block, [bf16])[0], False, -2)]
    projected, *others = forward([pieces[0], near, last], weight, block, [f32, bf16, bf16])
    returned += [shifted(other, False, -k) for other, k in zip(others, (1, 3), strict=True)]
    for other in returned:
        projected = projected + other.astype(f32)
    table_grads = accumulate(asked, arrived, rows, 2 * block)
    return (projected.astype(bf16), table_grads)


def solution(mesh):
    sides = (4, 4, 4, 2)
    torus = Mesh(mesh.devices.reshape(sides), (*AXES, "mp"))

    return jax.shard_map(
        on_device,
        mesh=torus,
        in_specs=(
            P(None, AXES, "mp"),
            P(None, "mp"),
            P(AXES),
            P(None, AXES, None),
            P(None, AXES),
            P(),
            P(AXES, "mp"),
            P(AXES, "mp"),
        ),
        out_specs=(P(AXES, "mp"), P(None, AXES, "mp")),
        check_vma=False,
    )
```

```python
import functools
import jax
import jax.numpy as jnp
from jax import lax
from jax.experimental import pallas as pl
from jax.experimental.pallas import tpu as pltpu
from jax.sharding import Mesh, PartitionSpec as P

eps = 1e-05
f32, bf16, i32 = jnp.float32, jnp.bfloat16, jnp.int32
LANES = 128
SPAN = 256
AXES = ("x", "y", "z")


def iota(shape, dim):
    return lax.broadcasted_iota(i32, shape, dim)


def dot(a, b, ca, cb):
    return lax.dot_general(a, b, (((ca,), (cb,)), ((), ())), preferred_element_type=f32)


def route_body(owner_ref, offset_ref, wanted_ref, slot_ref, *, groups, cap):
    ngram, _, tokens = owner_ref.shape
    earlier = (iota((tokens, tokens), 0) < iota((tokens, tokens), 1)).astype(f32).astype(bf16)
    lane = iota((groups, LANES), 1)
    wanted = jnp.full((groups, LANES), -1, i32)
    for k in range(ngram):
        owner = owner_ref[k]
        offset = offset_ref[k : k + 1, :]
        mine = jnp.broadcast_to(owner, (groups, tokens)) == iota((groups, tokens), 0)
        before = dot(mine.astype(f32).astype(bf16), earlier, 1, 0).astype(i32)
        rank = jnp.sum(jnp.where(mine, before, 0), axis=0, keepdims=True)
        slot_ref[k : k + 1, :] = owner * (ngram * cap) + k * cap + rank
        for r in range(cap):
            hit = jnp.where(mine & (before == r), offset + 1, 0)
            value = jnp.sum(hit, axis=1, keepdims=True) - 1
            wanted = jnp.where(lane == k * cap + r, value, wanted)
    wanted_ref[...] = wanted


def route(owner, offset, groups, cap):
    ngram, _, tokens = owner.shape
    return pl.pallas_call(
        functools.partial(route_body, groups=groups, cap=cap),
        out_shape=(
            jax.ShapeDtypeStruct((groups, LANES), i32),
            jax.ShapeDtypeStruct((ngram, tokens), i32),
        ),
        name="route",
    )(owner, offset)


def row_picks(asked, k, cap, rows):
    groups = asked.shape[0]
    total = groups * cap
    spread = (iota((total, groups), 0) // cap == iota((total, groups), 1)).astype(f32).astype(bf16)
    code = asked + 1
    high = (code >> 5).astype(f32).astype(bf16)
    low = (code & 31).astype(f32).astype(bf16)
    codes = dot(spread, high, 1, 0) * 32.0 + dot(spread, low, 1, 0)
    place = iota((total, LANES), 1) == k * cap + iota((total, LANES), 0) % cap
    column = jnp.sum(jnp.where(place, codes, 0.0), axis=1, keepdims=True).astype(i32) - 1
    return (column == iota((total, rows), 1)).astype(f32).astype(bf16)


def lookup_body(asked_ref, table_ref, out_ref, picks_ref, *, cap):
    k = pl.program_id(0)
    rows = table_ref.shape[1]

    @pl.when(pl.program_id(1) == 0)
    def _():
        picks_ref[...] = row_picks(asked_ref[...], k, cap, rows)

    out = dot(picks_ref[...], table_ref[0], 1, 0).astype(bf16)
    out_ref[...] = out.reshape(out_ref.shape)


def lookup(asked, tables, cap, block):
    groups = asked.shape[0]
    ngram, rows, width = tables.shape
    return pl.pallas_call(
        functools.partial(lookup_body, cap=cap),
        grid=(ngram, width // block),
        in_specs=[
            pl.BlockSpec((groups, LANES), lambda k, j: (0, 0)),
            pl.BlockSpec((1, rows, block), lambda k, j: (k, 0, j)),
        ],
        out_specs=pl.BlockSpec((groups, 1, cap, block), lambda k, j: (0, k, 0, j)),
        out_shape=jax.ShapeDtypeStruct((groups, ngram, cap, width), bf16),
        scratch_shapes=[pltpu.VMEM((groups * cap, rows), bf16)],
        name="lookup",
    )(asked, tables)


def slot_columns(slot_ref, slots):
    ngram, tokens = slot_ref.shape
    filled = jnp.concatenate([slot_ref[...], jnp.zeros((8 - ngram, tokens), i32)], axis=0)
    columns = filled.astype(f32).T.astype(i32)
    place = iota((tokens, slots), 1)
    hit = place == columns[:, 0:1]
    for k in range(1, ngram):
        hit = hit | (place == columns[:, k : k + 1])
    return hit.astype(f32).astype(bf16)


def side_by_side(ref):
    return jnp.concatenate([ref[i] for i in range(ref.shape[0])], axis=1)


def combine_body(
    slot_ref, ids_ref, fetched_ref, bytes_ref, out_ref, square_ref, picks_ref, codes_ref
):
    tokens, slots = picks_ref.shape

    @pl.when(pl.program_id(0) == 0)
    def _():
        picks_ref[...] = slot_columns(slot_ref, slots)
        vocab = codes_ref.shape[0]
        codes_ref[...] = (iota((vocab, tokens), 0) == ids_ref[...]).astype(f32).astype(bf16)
        square_ref[...] = jnp.zeros(square_ref.shape, f32)

    block = fetched_ref.shape[-1]
    fetched = fetched_ref[...].reshape(slots, block)
    summed = dot(picks_ref[...], fetched, 1, 0) + dot(codes_ref[...], bytes_ref[...], 0, 0)
    embedded = summed.astype(bf16)
    for i in range(block // SPAN):
        out_ref[i] = embedded[:, i * SPAN : (i + 1) * SPAN]
    values = embedded.astype(f32)
    square_ref[...] += jnp.sum(values * values, axis=1, keepdims=True)


def combine(slot, ids, fetched, byte_table, block):
    groups, ngram, cap, width = fetched.shape
    tokens = slot.shape[1]
    vocab = byte_table.shape[0]
    slots = groups * ngram * cap
    return pl.pallas_call(
        combine_body,
        grid=(width // block,),
        in_specs=[
            pl.BlockSpec((ngram, tokens), lambda j: (0, 0)),
            pl.BlockSpec((1, tokens), lambda j: (0, 0)),
            pl.BlockSpec((groups, ngram, cap, block), lambda j: (0, 0, 0, j)),
            pl.BlockSpec((vocab, block), lambda j: (0, j)),
        ],
        out_specs=(
            pl.BlockSpec((block // SPAN, tokens, SPAN), lambda j: (j, 0, 0)),
            pl.BlockSpec((tokens, LANES), lambda j: (0, 0)),
        ),
        out_shape=(
            jax.ShapeDtypeStruct((width // SPAN, tokens, SPAN), bf16),
            jax.ShapeDtypeStruct((tokens, LANES), f32),
        ),
        scratch_shapes=[pltpu.VMEM((tokens, slots), bf16), pltpu.VMEM((vocab, tokens), bf16)],
        name="combine",
    )(slot, ids.reshape(1, tokens), fetched, byte_table)


def dispatch_body(
    slot_ref, kept_ref, other_ref, gain_ref, embedded_ref, sq0_ref, sq1_ref, in0_ref, in1_ref, out_ref, picks_ref, *, full_width
):
    slots, tokens = picks_ref.shape

    @pl.when(pl.program_id(0) == 0)
    def _():
        place = iota((slots, tokens), 0)
        hit = place == slot_ref[0:1, :]
        for k in range(1, slot_ref.shape[0]):
            hit = hit | (place == slot_ref[k : k + 1, :])
        picks_ref[...] = hit.astype(f32).astype(bf16)

    scale = lax.rsqrt((sq0_ref[...] + sq1_ref[...])[:, 0:1] * (1.0 / full_width) + eps)
    inner = (in0_ref[...] + in1_ref[...])[:, 0:1] * (1.0 / full_width)
    values = side_by_side(embedded_ref).astype(f32)
    dnormed = side_by_side(kept_ref).astype(f32) + side_by_side(other_ref).astype(f32)
    scaled = dnormed * gain_ref[...]
    dembed = scale * scaled - values * (scale * scale * scale * inner)
    out = dot(picks_ref[...], dembed.astype(bf16), 1, 0).astype(bf16)
    out_ref[...] = out.reshape(out_ref.shape)


def dispatch(slot, kept, other, gain, embedded, sums, groups, cap, full_width, block):
    ngram, tokens = slot.shape
    width = embedded.shape[0] * SPAN
    slots = groups * ngram * cap
    blocked = pl.BlockSpec((block // SPAN, tokens, SPAN), lambda j: (j, 0, 0))
    total = pl.BlockSpec((tokens, LANES), lambda j: (0, 0))
    return pl.pallas_call(
        functools.partial(dispatch_body, full_width=full_width),
        grid=(width // block,),
        in_specs=[
            pl.BlockSpec((ngram, tokens), lambda j: (0, 0)),
            blocked,
            blocked,
            pl.BlockSpec((1, block), lambda j: (0, j)),
            blocked,
            total,
            total,
            total,
            total,
        ],
        out_specs=pl.BlockSpec((groups, ngram, cap, block), lambda j: (0, 0, 0, j)),
        out_shape=jax.ShapeDtypeStruct((groups, ngram, cap, width), bf16),
        scratch_shapes=[pltpu.VMEM((slots, tokens), bf16)],
        name="dispatch",
    )(slot, kept, other, gain, embedded, *sums)


def accumulate_body(asked_ref, arrived_ref, out_ref, picks_ref, *, cap):
    k = pl.program_id(0)
    rows = out_ref.shape[1]
    groups = asked_ref.shape[0]
    total = groups * cap

    @pl.when(pl.program_id(1) == 0)
    def _():
        spread = (iota((total, groups), 0) // cap == iota((total, groups), 1)).astype(f32).astype(bf16)
        code = asked_ref[...] + 1
        high = (code >> 5).astype(f32).astype(bf16)
        low = (code & 31).astype(f32).astype(bf16)
        codes = dot(high, spread, 0, 1) * 32.0 + dot(low, spread, 0, 1)
        place = iota((LANES, total), 0) == k * cap + iota((LANES, total), 1) % cap
        line = jnp.sum(jnp.where(place, codes, 0.0), axis=0, keepdims=True).astype(i32) - 1
        picks_ref[...] = (iota((rows, total), 0) == line).astype(f32).astype(bf16)

    arrived = arrived_ref[...].reshape(total, arrived_ref.shape[-1])
    out_ref[0] = dot(picks_ref[...], arrived, 1, 0).astype(bf16)


def accumulate(asked, arrived, rows, block):
    groups, ngram, cap, width = arrived.shape
    return pl.pallas_call(
        functools.partial(accumulate_body, cap=cap),
        grid=(ngram, width // block),
        in_specs=[
            pl.BlockSpec((groups, LANES), lambda k, j: (0, 0)),
            pl.BlockSpec((groups, 1, cap, block), lambda k, j: (0, k, 0, j)),
        ],
        out_specs=pl.BlockSpec((1, rows, block), lambda k, j: (k, 0, j)),
        out_shape=jax.ShapeDtypeStruct((ngram, rows, width), bf16),
        scratch_shapes=[pltpu.VMEM((rows, groups * cap), bf16)],
        name="accumulate",
    )(asked, arrived)


def exchange(array):
    return lax.all_to_all(array, AXES, split_axis=0, concat_axis=0, tiled=True)


def swapped(array):
    return lax.ppermute(array, "mp", [(0, 1), (1, 0)])


def shifted(array, turned, by):
    pairs = []
    for x in range(4):
        for y in range(4):
            for c in range(2):
                along_x = (c == 0) != turned
                to = ((x + by) % 4, y) if along_x else (x, (y + by) % 4)
                pairs.append(((x * 4 + y) * 2 + c, (to[0] * 4 + to[1]) * 2 + c))
    return lax.ppermute(array, ("x", "y", "mp"), pairs)


def shifted_z(array, by):
    return lax.ppermute(array, "z", [(i, (i + by) % 4) for i in range(4)])


def joined(blocks, here, dim):
    shape = list(blocks[0][0].shape)
    shape.insert(dim, 4)
    whole = jnp.zeros(shape, blocks[0][0].dtype)
    for block, away in blocks:
        whole = lax.dynamic_update_slice_in_dim(
            whole, jnp.expand_dims(block, dim), (here + away) % 4, dim
        )
    return whole


def product_body(*refs):
    cots, weight_ref, outs = refs[:4], refs[4], refs[5:]
    for cot_ref, out_ref in zip(cots, outs, strict=True):
        out_ref[...] = dot(cot_ref[...], weight_ref[...], 1, 1).astype(bf16)


def product(cots, weight, block):
    tokens, width = cots[0].shape
    rows = weight.shape[0]
    return pl.pallas_call(
        product_body,
        grid=(rows // block,),
        in_specs=[pl.BlockSpec((tokens, width), lambda j: (0, 0)) for _ in cots]
        + [pl.BlockSpec((block, width), lambda j: (j, 0))],
        out_specs=[pl.BlockSpec((tokens, block), lambda j: (0, j)) for _ in cots],
        out_shape=[jax.ShapeDtypeStruct((tokens, rows), bf16) for _ in cots],
        name="product",
    )(*cots, weight)


def forward_body(*refs):
    count = len(refs) // 2
    pieces, weight_ref, outs = refs[:count], refs[count], refs[count + 1 :]
    for piece_ref, out_ref in zip(pieces, outs, strict=True):
        out_ref[...] = dot(piece_ref[...], weight_ref[...], 1, 0).astype(out_ref.dtype)


def forward(pieces, weight, block, types):
    tokens, rows = pieces[0].shape
    width = weight.shape[1]
    return pl.pallas_call(
        forward_body,
        grid=(width // block,),
        in_specs=[pl.BlockSpec((tokens, rows), lambda j: (0, 0)) for _ in pieces]
        + [pl.BlockSpec((rows, block), lambda j: (0, j))],
        out_specs=[pl.BlockSpec((tokens, block), lambda j: (0, j)) for _ in pieces],
        out_shape=[jax.ShapeDtypeStruct((tokens, width), kind) for kind in types],
        name="forward",
    )(*pieces, weight)


def feature_block(core, quarter, i):
    return jnp.where(core == 0, 4 * quarter + i, 4 * i + quarter)


def settle_body(place_ref, own_ref, theirs_ref, gain_ref, mine_ref, other_ref, *refs, full_width):
    core, ring = place_ref[0], place_ref[1]
    quarters, (kept_ref, given_ref, inner_ref), pieces = refs[:4], refs[4:7], refs[7:]
    tokens = inner_ref.shape[0]
    scale = lax.rsqrt((mine_ref[...] + other_ref[...])[:, 0:1] * (1.0 / full_width) + eps)
    total = jnp.zeros((tokens, SPAN), f32)
    for k, ref in enumerate(quarters):
        quarter = (ring + 4 - k) % 4
        for i in range(4):
            at = feature_block(core, quarter, i)
            here, ours = at % 8, at // 8 == core
            lanes = slice(i * SPAN, (i + 1) * SPAN)
            piece = ref[:, lanes]
            gain = gain_ref[at]
            values = jnp.where(ours, own_ref[here].astype(f32), theirs_ref[here].astype(f32))
            total += values * (piece.astype(f32) * gain)
            pieces[(4 - k) % 4][:, lanes] = (values * scale * gain).astype(bf16)

            @pl.when(ours)
            def _():
                kept_ref[here] = piece

            @pl.when(jnp.logical_not(ours))
            def _():
                given_ref[here] = piece

    inner_ref[...] = jnp.broadcast_to(jnp.sum(total, axis=1, keepdims=True), inner_ref.shape)


def settle(place, own, theirs, gain, squares, quarters, full_width, block):
    tokens = own.shape[1]
    blocked = pl.BlockSpec((8, block, SPAN), lambda j: (0, j, 0))
    flat = pl.BlockSpec((block, 4 * SPAN), lambda j: (j, 0))
    total = pl.BlockSpec((block, LANES), lambda j: (j, 0))
    half = jax.ShapeDtypeStruct((8, tokens, SPAN), bf16)
    out = pl.pallas_call(
        functools.partial(settle_body, full_width=full_width),
        grid=(tokens // block,),
        in_specs=[
            pl.BlockSpec(memory_space=pltpu.SMEM),
            blocked,
            blocked,
            pl.BlockSpec((16, 1, SPAN), lambda j: (0, 0, 0)),
            total,
            total,
            *[flat] * 4,
        ],
        out_specs=[blocked, blocked, total, *[flat] * 4],
        out_shape=[
            half,
            half,
            jax.ShapeDtypeStruct((tokens, LANES), f32),
            *[jax.ShapeDtypeStruct((tokens, 4 * SPAN), bf16)] * 4,
        ],
        name="settle",
    )(place, own, theirs, gain.reshape(16, 1, SPAN), *squares, *quarters)
    return out[0], out[1], out[2], out[3:]


def on_device(
    hash_tables, byte_table, byte_ids, hash_owner, hash_offset, gain, proj_weight, cotangent
):
    groups = lax.axis_size(AXES)
    half = lax.axis_index("mp")
    first = half == 0
    x, y, z = (lax.axis_index(axis) for axis in AXES)
    ring, side = jnp.where(first, x, y), jnp.where(first, y, x)
    _, rows, width = hash_tables.shape
    tokens = byte_ids.shape[0]
    full_width = gain.shape[0]
    cap = 2 * tokens // groups
    block = 512

    gain_half = lax.dynamic_slice_in_dim(gain, half * width, width)[None, :]
    wanted, slot = route(jnp.swapaxes(hash_owner, 1, 2), hash_offset, groups, cap)
    asked = exchange(wanted.reshape(groups, 1, LANES)).reshape(groups, LANES)

    blocks = [(proj_weight, 0)] + [(shifted(proj_weight, True, -k), k) for k in (1, 3, 2)]
    weight = joined(blocks, side, 0)
    after, before = shifted_z(weight, -1), shifted_z(weight, 1)
    opposite = [shifted_z(after[:2], -1), shifted_z(before[2:], 1)]
    blocks = [(weight, 0), (after, 1), (before, 3), (jnp.concatenate(opposite), 2)]
    weight = joined(blocks, z, 1).reshape(-1, width)
    two, one, three = (shifted(cotangent, False, -k) for k in (2, 1, 3))
    cots = [cotangent, one, two, three]

    looked = lookup(asked, hash_tables, cap, 2 * block)
    fetched = exchange(looked)

    products = product(cots, weight, 256)
    quarters = [products[0]] + [shifted(products[k], False, k) for k in (1, 2, 3)]
    place = jnp.stack([half, ring]).astype(i32)
    embedded, square = combine(slot, byte_ids, fetched, byte_table, 2 * block)
    squares = (square, swapped(square))
    theirs = swapped(embedded)
    kept, given, inner, pieces = settle(
        place, embedded, theirs, gain, squares, quarters, full_width, tokens // 2
    )
    other = swapped(given)
    sums = (*squares, inner, swapped(inner))
    across, near, last = (shifted(pieces[k], False, k) for k in (2, 1, 3))
    sends = dispatch(slot, kept, other, gain_half, embedded, sums, groups, cap, full_width, 2 * block)
    arrived = exchange(sends)

    returned = [shifted(forward([across], weight, 2 * block, [bf16])[0], False, -2)]
    projected, *others = forward([pieces[0], near, last], weight, block, [f32, bf16, bf16])
    returned += [shifted(other, False, -k) for other, k in zip(others, (1, 3), strict=True)]
    for other in returned:
        projected = projected + other.astype(f32)
    table_grads = accumulate(asked, arrived, rows, 2 * block)
    return (projected.astype(bf16), table_grads)


def solution(mesh):
    sides = (4, 4, 4, 2)
    torus = Mesh(mesh.devices.reshape(sides), (*AXES, "mp"))

    return jax.shard_map(
        on_device,
        mesh=torus,
        in_specs=(
            P(None, AXES, "mp"),
            P(None, "mp"),
            P(AXES),
            P(None, AXES, None),
            P(None, AXES),
            P(),
            P(AXES, "mp"),
            P(AXES, "mp"),
        ),
        out_specs=(P(AXES, "mp"), P(None, AXES, "mp")),
        check_vma=False,
    )
```
